32 devices in a mesh: fov: 8 (over z, x), row: 4 (over y, core).
Axes of the slice: x: 2, y: 2, z: 4, core: 2. Of those that a mesh axis runs over, the one named last changes fastest.
Arguments:
- frames: bfloat16 [8, 5, 512, 512], P('fov', None, 'row'), parts along dimension 0, may hold values from 0.01 to 13, as said below
- phase_offset: float32 [8], P('fov'), parts along dimension 0, may hold values from -3.140625 to 3.140625
- order_gain: float32 [8, 5], P('fov'), parts along dimension 0, may hold values from 0.5 to 2
- band_shift: int32 [8, 2], P('fov'), parts along dimension 0, may hold values from -96 to 96
Outputs:
- picture: float32 [8192, 1024], P(('fov', 'row')), parts along dimension 0
The draws below stay inside these ranges and needn't reach their ends.
There are 8 independent parts, one for each index of `fov`. The reference program is written for one: setup_inputs(seed, part) draws one part's arguments, and reference() takes and returns one part's arrays. A program takes and returns all parts, laid end to end along the dimension named above; each array names one. Nothing has to cross between parts.
Inputs may be any that keep to these rules, and one draw needn't show every extreme that they name: `frames`: positive intensities. `band_shift`: offsets in frequency bins of the 1024-point grid, row component first.
All inputs are finite; a program needn't handle non-finite values.
Results may differ from the reference program's by a relative error of at most 0.0003.
Values sent between devices are 32-bit elements; how exact they have to be, the bound alone decides.
A program may use at most 128 MiB of HBM per device.

```python
import math
import jax
import jax.numpy as jnp
from jax import lax

PIX = 512
GRID = 1024
PHASES = 5
ANGLES = 1


def draw_frames(key, part):
    subkeys = jax.random.split(key, 4)
    frame_shape = (ANGLES, PHASES, PIX, PIX)
    levels = jax.random.uniform(subkeys[0], (ANGLES, PHASES, 1, 1), jnp.float32, 0.5, 2.0)
    slopes = jax.random.uniform(subkeys[1], (ANGLES, PHASES, 1, 1), jnp.float32, 0.6, 1.2)
    signs_draw = jnp.where(jax.random.bernoulli(subkeys[2], 0.5, (ANGLES, PHASES, 1, 1)), 1.0, -1.0)
    row_pos = (jnp.arange(PIX, dtype=jnp.float32) / PIX - 0.5).reshape(1, 1, PIX, 1)
    profile = jnp.exp(2.0 * slopes * signs_draw * row_pos)
    texture = jnp.clip(1.0 + 0.3 * jax.random.normal(subkeys[3], frame_shape, jnp.float32), 0.1, 1.9)
    return (levels * profile * texture).astype(jnp.bfloat16)


def setup_inputs(seed: int = 0, part: int = 0) -> dict:
    seeds = jax.random.split(jax.random.key(seed), 5)
    own_keys = jax.random.split(jax.random.fold_in(seeds[4], part), 5)
    frames = draw_frames(jax.random.fold_in(jax.random.fold_in(seeds[4], part), 71), part)
    phase_offset = jnp.clip(jax.random.uniform(own_keys[1], (ANGLES,), jnp.float32, -3.140625, 3.140625), -3.140625, 3.140625)
    order_gain = jnp.clip(jnp.exp(jax.random.uniform(own_keys[2], (ANGLES, PHASES), jnp.float32, math.log(0.5), math.log(2.0))), 0.5, 2.0)
    band_shift = jax.random.randint(own_keys[3], (ANGLES, 2), -(3 * PIX) // 16, (3 * PIX) // 16 + 1).astype(jnp.int32)
    return {"frames": frames, "phase_offset": phase_offset, "order_gain": order_gain, "band_shift": band_shift}


wiener = 0.1
gain_out = 8.0
cut_share = 0.45

def wrap_signed(values, length):
    return (values + length // 2) % length - length // 2

def transfer_curve(freq_y, freq_x, cutoff):
    float_y = freq_y.astype(jnp.float32)
    float_x = freq_x.astype(jnp.float32)
    radius = jnp.sqrt(float_y * float_y + float_x * float_x) / cutoff
    radius = jnp.minimum(radius, 1.0)
    return 2.0 / math.pi * (jnp.arccos(radius) - radius * jnp.sqrt(1.0 - radius * radius))

def reference(frames, phase_offset, order_gain, band_shift):
    intensity = frames.astype(jnp.float32)
    totals = lax.optimization_barrier(jnp.sum(intensity, axis=(2, 3)))
    scales = PIX * PIX / totals
    half_pix = PIX // 2
    cutoff = cut_share * PIX
    signed_index = wrap_signed(jnp.arange(PIX, dtype=jnp.int32), PIX)
    base_curve = transfer_curve(signed_index[:, None], signed_index[None, :], cutoff)
    fine_index = jnp.arange(GRID, dtype=jnp.int32)
    numerator = None
    denominator = jnp.full((GRID, GRID), wiener, jnp.float32)
    for angle_idx in range(ANGLES):
        phase_angle = 2.0 * math.pi * jnp.arange(PHASES, dtype=jnp.float32) / PHASES + phase_offset[angle_idx]
        weight = scales[angle_idx] / PHASES
        shift_y = band_shift[angle_idx, 0]
        shift_x = band_shift[angle_idx, 1]
        for order_idx in range(PHASES):
            order_val = order_idx - PHASES // 2
            coef_re = weight * jnp.cos(order_val * phase_angle)
            coef_im = -weight * jnp.sin(order_val * phase_angle)
            band_re = jnp.tensordot(coef_re, intensity[angle_idx], axes=1, precision=lax.Precision.HIGHEST)
            band_im = jnp.tensordot(coef_im, intensity[angle_idx], axes=1, precision=lax.Precision.HIGHEST)
            gain_val = order_gain[angle_idx, order_idx]
            spectrum = jnp.fft.fft2(lax.complex(band_re, band_im)) * (gain_val * base_curve)
            zero_block = jnp.zeros_like(spectrum)
            tall = jnp.concatenate([spectrum[:half_pix], zero_block, spectrum[half_pix:]], axis=0)
            zero_wide = jnp.zeros_like(tall)
            embedded = jnp.concatenate([tall[:, :half_pix], zero_wide, tall[:, half_pix:]], axis=1)
            moved = jnp.roll(jnp.roll(embedded, order_val * shift_y, axis=0), order_val * shift_x, axis=1)
            numerator = moved if numerator is None else numerator + moved
            shifted_curve = transfer_curve(wrap_signed(fine_index[:, None] - order_val * shift_y, GRID), wrap_signed(fine_index[None, :] - order_val * shift_x, GRID), cutoff)
            denominator = denominator + gain_val * gain_val * shifted_curve * shifted_curve
    picture = jnp.fft.ifft2(numerator / denominator)
    return (gain_out * jnp.real(picture)).astype(jnp.float32)
```

```python
import functools
import math

import jax
import jax.numpy as jnp
import numpy as np
from jax import lax
from jax.experimental import pallas as pl
from jax.experimental.pallas import tpu as pltpu
from jax.sharding import PartitionSpec as P

MESH = pl.DeviceIdType.MESH
wiener = 0.1
gain_out = 8.0
cut_share = 0.45
CORES = 2


def split_table(table):
    high = table.astype(np.float32).astype(jnp.bfloat16)
    low = (table - high.astype(np.float64)).astype(np.float32).astype(jnp.bfloat16)
    return np.stack([high, low])


def cos_sin(points, freqs, length):
    angle = 2.0 * math.pi * ((points[:, None] * freqs[None, :]) % length) / length
    return np.cos(angle), np.sin(angle)


def tables(pixels, count):
    half = pixels // 2
    share = half // count
    chips = count // CORES
    points = np.arange(pixels)
    freqs = np.arange(half)
    alternate = 1.0 - 2.0 * (points % 2)
    cos_f, sin_f = cos_sin(points, freqs, pixels)
    sin_f[:, 0] = alternate

    def by_device(cos_part, sin_part):
        rows = cos_part.shape[0]
        both = np.stack([cos_part.reshape(rows, count, share), sin_part.reshape(rows, count, share)], axis=2)
        return both.reshape(rows, count * 2 * share)

    width = CORES * 2 * share
    lead = by_device(cos_f, sin_f).reshape(pixels, chips, width).transpose(1, 0, 2)
    column = np.concatenate([cos_f, sin_f], axis=1).T
    column = column.reshape(pixels, chips, pixels // chips).transpose(1, 0, 2)
    inverse = []
    for odd in range(2):
        cos_i, sin_i = cos_sin(2 * points + odd, freqs, 2 * pixels)
        sin_i[:, 0] = alternate
        inverse.append(np.concatenate([cos_i, sin_i], axis=1))
    inverse = np.stack(inverse)
    wide = np.arange(2 * pixels)
    cos_w, sin_w = cos_sin(wide, freqs, 2 * pixels)
    sin_w[:, 0] = 1.0 - 2.0 * ((wide // 2) % 2)
    last = by_device(cos_w, sin_w).T.reshape(chips, width, 2 * pixels)
    return tuple(split_table(t) for t in (lead, column, inverse, last))


def otf_polynomial():
    nodes = 0.5 + 0.5 * np.cos(math.pi * (np.arange(64) + 0.5) / 64)
    nodes = np.minimum(nodes, 0.9985)
    root = np.sqrt(1 - nodes * nodes)
    values = 2 / math.pi * (np.arccos(nodes) - nodes * root) / root**3
    fit = np.polynomial.chebyshev.Chebyshev.fit(nodes, values, 10, domain=[0, 1])
    poly = fit.convert(kind=np.polynomial.Polynomial).coef
    return [float(c) for c in poly[::-1]]


def halves(value):
    high = value.astype(jnp.bfloat16)
    return high, (value - high.astype(jnp.float32)).astype(jnp.bfloat16)


def dot(left, right):
    return jnp.dot(left, right, preferred_element_type=jnp.float32)


def dot3(left_hi, left_lo, right_hi, right_lo):
    return dot(left_hi, right_hi) + (dot(left_hi, right_lo) + dot(left_lo, right_hi))


def kernel(count, poly, frames, offset, gain, shift, lead_h, column_h, inverse_h, last_h, out,
           lead, column, inverse, last, tot_send, tot, planes, send1, recv1, mixed, weights, coef,
           send2, recv2, woven, table_sem, tot_ss, tot_rs, ss1, rs1, ss2, rs2):
    me = lax.axis_index("row")
    chips = count // CORES
    chip, core = me // CORES, me % CORES
    phases, rows, pixels = frames.shape[1:]
    half = pixels // 2
    share = half // count
    lanes = 2 * share
    others = [lax.rem(me + step, count) for step in range(1, count)]
    far_chips = [lax.rem(chip + step, chips) for step in range(1, chips)]
    sibling = chip * CORES + 1 - core
    far = [(c, c * CORES + k) for c in far_chips for k in range(CORES)]

    loads = []
    for idx, (source, target) in enumerate(
        ((lead_h, lead), (column_h, column), (inverse_h, inverse), (last_h, last))
    ):
        loads.append(pltpu.make_async_copy(source, target, table_sem.at[idx]))
    loads[0].start()

    lane8 = lax.broadcasted_iota(jnp.int32, (8, 128), 1)
    part = jnp.zeros((8, 128), jnp.float32)
    for p in range(phases):
        f = frames[0, p].astype(jnp.float32)
        s = jnp.sum(jnp.sum(f, axis=0, keepdims=True), axis=1, keepdims=True)
        part = part + jnp.where(lane8 == p, s, 0.0)
    tot_send[...] = part
    tot[me] = part

    barrier = pltpu.get_barrier_semaphore()
    for peer in others:
        pl.semaphore_signal(barrier, inc=1, device_id={"row": peer}, device_id_type=MESH)
    pl.semaphore_wait(barrier, count - 1)

    def tot_copy(peer, slot):
        return pltpu.make_async_remote_copy(
            src_ref=tot_send, dst_ref=tot.at[slot], send_sem=tot_ss.at[peer], recv_sem=tot_rs.at[slot],
            device_id={"row": peer}, device_id_type=MESH)

    for peer in others:
        tot_copy(peer, me).start()
    for load in loads[1:]:
        load.start()

    shift_y, shift_x = shift[0, 0], shift[0, 1]
    inv_cut = 1.0 / (cut_share * pixels)
    scale_out = gain_out / (4.0 * pixels * pixels)

    def wrap(value):
        return ((value + half) & (pixels - 1)) - half

    def lane_freq(shape):
        lane = lax.broadcasted_iota(jnp.int32, shape, 1)
        base = me * share
        plus = base + lane
        minus = base + lane - share
        minus = jnp.where(minus == 0, -half, minus)
        return jnp.where(lane < share, plus, -minus)

    def row_freq(first, sign, shape):
        row = first + lax.broadcasted_iota(jnp.int32, shape, 0)
        if sign == 0:
            return row
        return jnp.where(row == 0, half, -row)

    def placed(freq, order, shift_val):
        return order * shift_val + wrap(freq - order * shift_val)

    def curve(sq_y, sq_x):
        t = jnp.minimum(sq_y + sq_x, 1.0)
        r = t * lax.rsqrt(jnp.maximum(t, 1e-30))
        u = 1.0 - t
        v = u * lax.rsqrt(jnp.maximum(u, 1e-30))
        acc = jnp.full(t.shape, poly[0], jnp.float32)
        for c in poly[1:]:
            acc = acc * r + c
        return acc * (u * v)

    step = 16
    orders = phases // 2 + 1
    mid = phases // 2
    gains = [gain[0, j] for j in range(phases)]

    def make_weights(order):
        big_x = placed(lane_freq((step, lanes)), order, shift_x)
        sq_xs = []
        for j in range(phases):
            fx = (big_x - (j - mid) * shift_x).astype(jnp.float32) * inv_cut
            sq_xs.append(fx * fx)

        def body(i, carry):
            first = pl.multiple_of(i * step, step)
            for sign in range(2):
                big_y = placed(row_freq(first, sign, (step, lanes)), order, shift_y)
                den = jnp.full((step, lanes), wiener, jnp.float32)
                den_m = jnp.full((step, lanes), wiener, jnp.float32)
                own = None
                for j in range(phases):
                    fy = (big_y - (j - mid) * shift_y).astype(jnp.float32) * inv_cut
                    value = curve(fy * fy, sq_xs[j])
                    sq = value * value
                    den = den + (gains[j] * gains[j]) * sq
                    den_m = den_m + (gains[phases - 1 - j] * gains[phases - 1 - j]) * sq
                    if j == mid + order:
                        own = value
                if order == 0:
                    w = own * (gains[mid] * scale_out) / den
                else:
                    w = own * scale_out * (gains[mid + order] / den + gains[mid - order] / den_m)
                weights[order, sign, pl.ds(first, step), :] = w
            return carry

        lax.fori_loop(0, half // step, body, 0)

    make_weights(0)

    for peer in others:
        tot_copy(peer, peer).wait_recv()
    total = tot[0]
    for d in range(1, count):
        total = total + tot[d]
    level = jnp.where(lane8 < phases, float(pixels * pixels), 0.0) / jnp.where(lane8 < phases, total, 1.0)
    level = level / phases
    angle = 2.0 * math.pi / phases * lane8.astype(jnp.float32) + offset[0]

    col = lax.broadcasted_iota(jnp.int32, (8, pixels), 1)
    row = lax.broadcasted_iota(jnp.int32, (rows, 128), 0) + me * rows
    turn = 2.0 * math.pi / pixels

    groups = [(0, 2), (2, 2), (4, 1)]

    def send1_copy(dest, slot_chip, slot_core, source, g):
        first, wide = groups[g]
        window = pl.ds(first * lanes, wide * lanes)
        return pltpu.make_async_remote_copy(
            src_ref=send1.at[dest, :, window],
            dst_ref=recv1.at[slot_chip, pl.ds(pl.multiple_of(slot_core * rows, rows), rows), window],
            send_sem=ss1.at[dest, g], recv_sem=rs1.at[source, g],
            device_id={"row": dest}, device_id_type=MESH)

    loads[0].wait()
    for g, (first, wide) in enumerate(groups):
        order = 0 if wide == 1 else g + 1
        coef_re = level * jnp.cos(order * angle)
        if order == 0:
            band = coef_re[:1, 0:1] * frames[0, 0].astype(jnp.float32)
            for p in range(1, phases):
                band = band + coef_re[:1, p:p + 1] * frames[0, p].astype(jnp.float32)
            parts = [band]
        else:
            coef_im = -level * jnp.sin(order * angle)
            band_re = coef_re[:1, 0:1] * frames[0, 0].astype(jnp.float32)
            band_im = coef_im[:1, 0:1] * frames[0, 0].astype(jnp.float32)
            for p in range(1, phases):
                f = frames[0, p].astype(jnp.float32)
                band_re = band_re + coef_re[:1, p:p + 1] * f
                band_im = band_im + coef_im[:1, p:p + 1] * f
            arg_x = ((col * (order * shift_x)) & (pixels - 1)).astype(jnp.float32) * turn
            arg_y = ((row * (order * shift_y)) & (pixels - 1)).astype(jnp.float32) * turn
            cx, sx = jnp.cos(arg_x)[:1], jnp.sin(arg_x)[:1]
            cy, sy = jnp.cos(arg_y)[:, :1], jnp.sin(arg_y)[:, :1]
            ph_re = cy * cx - sy * sx
            ph_im = cy * sx + sy * cx
            parts = [band_re * ph_re - band_im * ph_im, band_re * ph_im + band_im * ph_re]
        for k, value in enumerate(parts):
            hi, lo = halves(value)
            planes[0, pl.ds((first + k) * rows, rows), :] = hi
            planes[1, pl.ds((first + k) * rows, rows), :] = lo
        span = pl.ds(first * rows, wide * rows)
        for c in far_chips:
            result = dot3(planes[0, span, :], planes[1, span, :], lead[0, c], lead[1, c])
            for k in range(wide):
                for kc in range(CORES):
                    send1[c * CORES + kc, :, pl.ds((first + k) * lanes, lanes)] = result[
                        k * rows:(k + 1) * rows, kc * lanes:(kc + 1) * lanes]
            for kc in range(CORES):
                send1_copy(c * CORES + kc, chip, core, me, g).start()
    mine = pl.ds(pl.multiple_of(core * rows, rows), rows)
    for g, (first, wide) in enumerate(groups):
        span = pl.ds(first * rows, wide * rows)
        result = dot3(planes[0, span, :], planes[1, span, :], lead[0, chip], lead[1, chip])
        for k in range(wide):
            block = result[k * rows:(k + 1) * rows]
            low_half, high_half = block[:, :lanes], block[:, lanes:]
            window = pl.ds((first + k) * lanes, lanes)
            recv1[chip, mine, window] = jnp.where(core == 0, low_half, high_half)
            send1[sibling, :, window] = jnp.where(core == 0, high_half, low_half)
        send1_copy(sibling, chip, core, me, g).start()

    for order in range(1, orders):
        make_weights(order)

    loads[1].wait()
    for g, (first, wide) in enumerate(groups):
        window = pl.ds(first * lanes, wide * lanes)
        send1_copy(sibling, chip, 1 - core, sibling, g).wait_recv()
        hi, lo = halves(recv1[chip, :, window])
        mixed[:, window] = dot3(column[0, chip], column[1, chip], hi, lo)
    for c in far_chips:
        for g, (first, wide) in enumerate(groups):
            window = pl.ds(first * lanes, wide * lanes)
            for kc in range(CORES):
                send1_copy(c * CORES + kc, c, kc, c * CORES + kc, g).wait_recv()
            hi, lo = halves(recv1[c, :, window])
            mixed[:, window] += dot3(column[0, c], column[1, c], hi, lo)

    lane = lax.broadcasted_iota(jnp.int32, (step, lanes), 1)
    low_lanes = lane < share
    special = jnp.logical_and(me == 0, jnp.logical_or(lane == 0, lane == share))
    special_top = jnp.logical_and(special, lane == share)
    freq_x = lane_freq((step, lanes))
    sign_x = jnp.where(low_lanes, 1.0, -1.0)
    parity_x = []
    for order in range(orders):
        turns = (placed(freq_x, order, shift_x) - freq_x) // pixels
        parity_x.append((1 - 2 * (turns & 1)).astype(jnp.float32))

    def turn_lanes(value):
        return pltpu.roll(value, share, 1)

    def combine(i, carry):
        first = pl.multiple_of(i * step, step)
        row0 = (first + lax.broadcasted_iota(jnp.int32, (step, lanes), 0)) == 0
        spectra = []
        for plane in range(phases):
            window = pl.ds(plane * lanes, lanes)
            upper = mixed[pl.ds(first, step), window]
            lower = mixed[pl.ds(half + first, step), window]
            upper_t, lower_t = turn_lanes(upper), turn_lanes(lower)
            as_is = jnp.logical_or(low_lanes, special)
            cc = jnp.where(as_is, upper, upper_t)
            sc = jnp.where(as_is, lower, lower_t)
            cs = jnp.where(special, 0.0, jnp.where(low_lanes, upper_t, upper)) * sign_x
            ss = jnp.where(special, 0.0, jnp.where(low_lanes, lower_t, lower)) * sign_x
            plus = (jnp.where(row0, cc, cc - ss), -jnp.where(row0, cs, sc + cs))
            minus = (jnp.where(row0, sc, cc + ss), jnp.where(row0, -ss, sc - cs))
            spectra.append((plus, minus))
        terms = []
        for sign in range(2):
            freq_y = row_freq(first, sign, (step, lanes))
            for order in range(orders):
                if order == 0:
                    re, im = spectra[phases - 1][sign]
                else:
                    rr, ri = spectra[2 * order - 2][sign]
                    ir, ii = spectra[2 * order - 1][sign]
                    re, im = rr - ii, ri + ir
                w = weights[order, sign, pl.ds(first, step), :]
                turns = (placed(freq_y, order, shift_y) - freq_y) // pixels
                terms.append((re * w, im * w, (1 - 2 * (turns & 1)).astype(jnp.float32)))
        for a in range(2):
            for b in range(2):
                sums = []
                for sign in range(2):
                    tot_re, tot_im = None, None
                    for order in range(orders):
                        re, im, par_y = terms[sign * orders + order]
                        factor = None
                        if a:
                            factor = par_y
                        if b:
                            factor = parity_x[order] if factor is None else factor * parity_x[order]
                        if factor is not None:
                            re, im = re * factor, im * factor
                        tot_re = re if tot_re is None else tot_re + re
                        tot_im = im if tot_im is None else tot_im + im
                    sums.append((tot_re, tot_im))
                (pr, pi), (mr, mi) = sums
                even_r = jnp.where(row0, pr, pr + mr)
                even_i = jnp.where(row0, pi, pi + mi)
                if a == 0:
                    odd_r = jnp.where(row0, mi, pr - mr)
                    odd_i = jnp.where(row0, -mr, pi - mi)
                else:
                    odd_r = jnp.where(row0, mr, pr - mr)
                    odd_i = jnp.where(row0, mi, pi - mi)

                def fold(x, y):
                    lo_val = x + turn_lanes(x)
                    hi_val = y - turn_lanes(y)
                    res = jnp.where(low_lanes, lo_val, hi_val)
                    res = jnp.where(special, x, res)
                    if b:
                        res = jnp.where(special_top, -y, res)
                    return res

                upper = fold(even_r, even_i)
                lower = fold(-odd_i, odd_r)
                window = pl.ds(b * lanes, lanes)
                hi, lo = halves(upper)
                coef[0, a, pl.ds(first, step), window] = hi
                coef[1, a, pl.ds(first, step), window] = lo
                hi, lo = halves(lower)
                coef[0, a, pl.ds(half + first, step), window] = hi
                coef[1, a, pl.ds(half + first, step), window] = lo
        return carry

    lax.fori_loop(0, half // step, combine, 0)

    def send2_copy(dest, slot_chip, slot_core, source, a):
        block = pl.ds(a * rows, rows)
        return pltpu.make_async_remote_copy(
            src_ref=send2.at[dest, :, block, :],
            dst_ref=recv2.at[slot_chip, :, block, pl.ds(pl.multiple_of(slot_core * lanes, lanes), lanes)],
            send_sem=ss2.at[dest, a], recv_sem=rs2.at[source, a],
            device_id={"row": dest}, device_id_type=MESH)

    loads[2].wait()
    for a in range(2):
        for _, dest in far:
            t = pl.ds(pl.multiple_of(dest * rows, rows), rows)
            result = dot3(inverse[0, a, t, :], inverse[1, a, t, :], coef[0, a], coef[1, a])
            for b in range(2):
                send2[dest, b, pl.ds(a * rows, rows), :] = result[:, b * lanes:(b + 1) * lanes]
            send2_copy(dest, chip, core, me, a).start()
    slot = pl.ds(pl.multiple_of(core * lanes, lanes), lanes)
    for a in range(2):
        for dest in (sibling, me):
            t = pl.ds(pl.multiple_of(dest * rows, rows), rows)
            result = dot3(inverse[0, a, t, :], inverse[1, a, t, :], coef[0, a], coef[1, a])
            for b in range(2):
                piece = result[:, b * lanes:(b + 1) * lanes]
                if dest is me:
                    recv2[chip, b, pl.ds(a * rows, rows), slot] = piece
                else:
                    send2[dest, b, pl.ds(a * rows, rows), :] = piece
            if dest is not me:
                send2_copy(dest, chip, core, me, a).start()

    loads[3].wait()
    for a in range(2):
        send2_copy(sibling, chip, 1 - core, sibling, a).wait_recv()
    wide_step = 256
    even_lane = (lax.broadcasted_iota(jnp.int32, (rows, wide_step), 1) & 1) == 0
    for stage, c in enumerate([chip] + far_chips):
        for a in range(2):
            if stage:
                for kc in range(CORES):
                    send2_copy(c * CORES + kc, c, kc, c * CORES + kc, a).wait_recv()
            block = pl.ds(a * rows, rows)
            for x in range(0, 2 * pixels, wide_step):
                span = pl.ds(x, wide_step)
                values = []
                for b in range(2):
                    hi, lo = halves(recv2[c, b, block, :])
                    values.append(dot3(hi, lo, last[0, c, :, span], last[1, c, :, span]))
                value = jnp.where(even_lane, values[0], values[1])
                place = pl.ds(a, rows, stride=2)
                for k in range(wide_step // 128):
                    piece = value[:, k * 128:(k + 1) * 128]
                    tile = x // 128 + k
                    if stage:
                        piece = piece + woven[tile, place, :]
                    woven[tile, place, :] = piece
    for tile in range(2 * pixels // 128):
        out[:, pl.ds(tile * 128, 128)] = woven[tile]

    for peer in others:
        tot_copy(peer, me).wait_send()
        for g in range(len(groups)):
            send1_copy(peer, chip, core, me, g).wait_send()
        for a in range(2):
            send2_copy(peer, chip, core, me, a).wait_send()


def solution(mesh):
    count = mesh.shape["row"]

    def per_device(frames, phase_offset, order_gain, band_shift):
        phases, rows, pixels = frames.shape[1:]
        lanes = pixels // count
        chips = count // CORES
        lead, column, inverse, last = tables(pixels, count)
        vmem = pl.BlockSpec(memory_space=pltpu.VMEM)
        smem = pl.BlockSpec(memory_space=pltpu.SMEM)
        hbm = pl.BlockSpec(memory_space=pl.ANY)
        bf16, f32 = jnp.bfloat16, jnp.float32
        dma = pltpu.SemaphoreType.DMA
        return pl.pallas_call(
            functools.partial(kernel, count, otf_polynomial()),
            out_shape=jax.ShapeDtypeStruct((2 * rows, 2 * pixels), f32),
            in_specs=[vmem, smem, smem, smem, hbm, hbm, hbm, hbm],
            out_specs=vmem,
            scratch_shapes=[
                pltpu.VMEM(lead.shape, bf16),
                pltpu.VMEM(column.shape, bf16),
                pltpu.VMEM(inverse.shape, bf16),
                pltpu.VMEM(last.shape, bf16),
                pltpu.VMEM((8, 128), f32),
                pltpu.VMEM((count, 8, 128), f32),
                pltpu.VMEM((2, phases * rows, pixels), bf16),
                pltpu.VMEM((count, rows, phases * lanes), f32),
                pltpu.VMEM((chips, CORES * rows, phases * lanes), f32),
                pltpu.VMEM((pixels, phases * lanes), f32),
                pltpu.VMEM((phases // 2 + 1, 2, pixels // 2, lanes), f32),
                pltpu.VMEM((2, 2, pixels, 2 * lanes), bf16),
                pltpu.VMEM((count, 2, 2 * rows, lanes), f32),
                pltpu.VMEM((chips, 2, 2 * rows, CORES * lanes), f32),
                pltpu.VMEM((2 * pixels // 128, 2 * rows, 128), f32),
                dma((4,)),
                dma((count,)), dma((count,)),
                dma((count, 3)), dma((count, 3)),
                dma((count, 2)), dma((count, 2)),
            ],
            compiler_params=pltpu.CompilerParams(
                collective_id=0, has_side_effects=True, vmem_limit_bytes=60000000
            ),
        )(frames, phase_offset, order_gain, band_shift,
          jnp.asarray(lead), jnp.asarray(column), jnp.asarray(inverse), jnp.asarray(last))

    in_specs = (P("fov", None, "row", None), P("fov"), P("fov", None), P("fov", None))
    return jax.shard_map(
        per_device, mesh=mesh, in_specs=in_specs, out_specs=P(("fov", "row"), None), check_vma=False
    )
```

```python
import functools
import math

import jax
import jax.numpy as jnp
import numpy as np
from jax import lax
from jax.experimental import pallas as pl
from jax.experimental.pallas import tpu as pltpu
from jax.sharding import PartitionSpec as P

MESH = pl.DeviceIdType.MESH
wiener = 0.1
gain_out = 8.0
cut_share = 0.45
CORES = 2


def split_table(table):
    high = table.astype(np.float32).astype(jnp.bfloat16)
    low = (table - high.astype(np.float64)).astype(np.float32).astype(jnp.bfloat16)
    return np.stack([high, low])


def cos_sin(points, freqs, length):
    angle = 2.0 * math.pi * ((points[:, None] * freqs[None, :]) % length) / length
    return np.cos(angle), np.sin(angle)


def tables(pixels, count):
    half = pixels // 2
    share = half // count
    chips = count // CORES
    points = np.arange(pixels)
    freqs = np.arange(half)
    alternate = 1.0 - 2.0 * (points % 2)
    cos_f, sin_f = cos_sin(points, freqs, pixels)
    sin_f[:, 0] = alternate

    def by_device(cos_part, sin_part):
        rows = cos_part.shape[0]
        both = np.stack([cos_part.reshape(rows, count, share), sin_part.reshape(rows, count, share)], axis=2)
        return both.reshape(rows, count * 2 * share)

    width = CORES * 2 * share
    lead = by_device(cos_f, sin_f).reshape(pixels, chips, width).transpose(1, 0, 2)
    column = np.concatenate([cos_f, sin_f], axis=1).T
    column = column.reshape(pixels, chips, pixels // chips).transpose(1, 0, 2)
    inverse = []
    for odd in range(2):
        cos_i, sin_i = cos_sin(2 * points + odd, freqs, 2 * pixels)
        sin_i[:, 0] = alternate
        inverse.append(np.concatenate([cos_i, sin_i], axis=1))
    inverse = np.stack(inverse)
    wide = np.arange(2 * pixels)
    cos_w, sin_w = cos_sin(wide, freqs, 2 * pixels)
    sin_w[:, 0] = 1.0 - 2.0 * ((wide // 2) % 2)
    last = by_device(cos_w, sin_w).T.reshape(chips, width, 2 * pixels)
    return tuple(split_table(t) for t in (lead, column, inverse, last))


def otf_polynomial():
    nodes = 0.5 + 0.5 * np.cos(math.pi * (np.arange(64) + 0.5) / 64)
    nodes = np.minimum(nodes, 0.9985)
    root = np.sqrt(1 - nodes * nodes)
    values = 2 / math.pi * (np.arccos(nodes) - nodes * root) / root**3
    fit = np.polynomial.chebyshev.Chebyshev.fit(nodes, values, 10, domain=[0, 1])
    poly = fit.convert(kind=np.polynomial.Polynomial).coef
    return [float(c) for c in poly[::-1]]


def halves(value):
    high = value.astype(jnp.bfloat16)
    return high, (value - high.astype(jnp.float32)).astype(jnp.bfloat16)


def dot(left, right):
    return jnp.dot(left, right, preferred_element_type=jnp.float32)


def dot3(left_hi, left_lo, right_hi, right_lo):
    return dot(left_hi, right_hi) + (dot(left_hi, right_lo) + dot(left_lo, right_hi))


def kernel(count, poly, frames, offset, gain, shift, lead_h, column_h, inverse_h, last_h, out,
           lead, column, inverse, last, tot_send, tot, planes, send1, recv1, mixed, weights, coef,
           send2, recv2, woven, table_sem, tot_ss, tot_rs, ss1, rs1, ss2, rs2):
    me = lax.axis_index("row")
    chips = count // CORES
    chip, core = me // CORES, me % CORES
    phases, rows, pixels = frames.shape[1:]
    half = pixels // 2
    share = half // count
    lanes = 2 * share
    others = [lax.rem(me + step, count) for step in range(1, count)]
    far_chips = [lax.rem(chip + step, chips) for step in range(1, chips)]
    sibling = chip * CORES + 1 - core
    far = [(c, c * CORES + k) for c in far_chips for k in range(CORES)]

    loads = []
    for idx, (source, target) in enumerate(
        ((lead_h, lead), (column_h, column), (inverse_h, inverse), (last_h, last))
    ):
        loads.append(pltpu.make_async_copy(source, target, table_sem.at[idx]))
    loads[0].start()

    lane8 = lax.broadcasted_iota(jnp.int32, (8, 128), 1)
    part = jnp.zeros((8, 128), jnp.float32)
    for p in range(phases):
        f = frames[0, p].astype(jnp.float32)
        s = jnp.sum(jnp.sum(f, axis=0, keepdims=True), axis=1, keepdims=True)
        part = part + jnp.where(lane8 == p, s, 0.0)
    tot_send[...] = part
    tot[me] = part

    barrier = pltpu.get_barrier_semaphore()
    for peer in others:
        pl.semaphore_signal(barrier, inc=1, device_id={"row": peer}, device_id_type=MESH)
    pl.semaphore_wait(barrier, count - 1)

    def tot_copy(peer, slot):
        return pltpu.make_async_remote_copy(
            src_ref=tot_send, dst_ref=tot.at[slot], send_sem=tot_ss.at[peer], recv_sem=tot_rs.at[slot],
            device_id={"row": peer}, device_id_type=MESH)

    for peer in others:
        tot_copy(peer, me).start()
    for load in loads[1:]:
        load.start()

    shift_y, shift_x = shift[0, 0], shift[0, 1]
    inv_cut = 1.0 / (cut_share * pixels)
    scale_out = gain_out / (4.0 * pixels * pixels)

    def wrap(value):
        return ((value + half) & (pixels - 1)) - half

    def lane_freq(shape):
        lane = lax.broadcasted_iota(jnp.int32, shape, 1)
        base = me * share
        plus = base + lane
        minus = base + lane - share
        minus = jnp.where(minus == 0, -half, minus)
        return jnp.where(lane < share, plus, -minus)

    def row_freq(first, sign, shape):
        row = first + lax.broadcasted_iota(jnp.int32, shape, 0)
        if sign == 0:
            return row
        return jnp.where(row == 0, half, -row)

    def placed(freq, order, shift_val):
        return order * shift_val + wrap(freq - order * shift_val)

    def curve(sq_y, sq_x):
        t = jnp.minimum(sq_y + sq_x, 1.0)
        r = t * lax.rsqrt(jnp.maximum(t, 1e-30))
        u = 1.0 - t
        v = u * lax.rsqrt(jnp.maximum(u, 1e-30))
        acc = jnp.full(t.shape, poly[0], jnp.float32)
        for c in poly[1:]:
            acc = acc * r + c
        return acc * (u * v)

    step = 16
    orders = phases // 2 + 1
    mid = phases // 2
    gains = [gain[0, j] for j in range(phases)]

    def make_weights(order):
        big_x = placed(lane_freq((step, lanes)), order, shift_x)
        sq_xs = []
        for j in range(phases):
            fx = (big_x - (j - mid) * shift_x).astype(jnp.float32) * inv_cut
            sq_xs.append(fx * fx)

        def body(i, carry):
            first = pl.multiple_of(i * step, step)
            for sign in range(2):
                big_y = placed(row_freq(first, sign, (step, lanes)), order, shift_y)
                den = jnp.full((step, lanes), wiener, jnp.float32)
                den_m = jnp.full((step, lanes), wiener, jnp.float32)
                own = None
                for j in range(phases):
                    fy = (big_y - (j - mid) * shift_y).astype(jnp.float32) * inv_cut
                    value = curve(fy * fy, sq_xs[j])
                    sq = value * value
                    den = den + (gains[j] * gains[j]) * sq
                    den_m = den_m + (gains[phases - 1 - j] * gains[phases - 1 - j]) * sq
                    if j == mid + order:
                        own = value
                if order == 0:
                    w = own * (gains[mid] * scale_out) / den
                else:
                    w = own * scale_out * (gains[mid + order] / den + gains[mid - order] / den_m)
                weights[order, sign, pl.ds(first, step), :] = w
            return carry

        lax.fori_loop(0, half // step, body, 0)

    col = lax.broadcasted_iota(jnp.int32, (8, pixels), 1)
    row = lax.broadcasted_iota(jnp.int32, (rows, 128), 0) + me * rows
    turn = 2.0 * math.pi / pixels
    waves = {}
    for order in range(1, orders):
        arg_x = ((col * (order * shift_x)) & (pixels - 1)).astype(jnp.float32) * turn
        arg_y = ((row * (order * shift_y)) & (pixels - 1)).astype(jnp.float32) * turn
        waves[order] = (jnp.cos(arg_x)[:1], jnp.sin(arg_x)[:1], jnp.cos(arg_y)[:, :1], jnp.sin(arg_y)[:, :1])
    angle = 2.0 * math.pi / phases * lane8.astype(jnp.float32) + offset[0]
    unmix = {order: (jnp.cos(order * angle), jnp.sin(order * angle)) for order in range(orders)}

    for peer in others:
        tot_copy(peer, peer).wait_recv()
    total = tot[0]
    for d in range(1, count):
        total = total + tot[d]
    level = jnp.where(lane8 < phases, float(pixels * pixels), 0.0) / jnp.where(lane8 < phases, total, 1.0)
    level = level / phases

    groups = [(0, 2), (2, 2), (4, 1)]

    def send1_copy(dest, slot_chip, slot_core, source, g):
        first, wide = groups[g]
        window = pl.ds(first * lanes, wide * lanes)
        return pltpu.make_async_remote_copy(
            src_ref=send1.at[dest, :, window],
            dst_ref=recv1.at[slot_chip, pl.ds(pl.multiple_of(slot_core * rows, rows), rows), window],
            send_sem=ss1.at[dest, g], recv_sem=rs1.at[source, g],
            device_id={"row": dest}, device_id_type=MESH)

    loads[0].wait()
    for g, (first, wide) in enumerate(groups):
        order = 0 if wide == 1 else g + 1
        coef_re = level * unmix[order][0]
        if order == 0:
            band = coef_re[:1, 0:1] * frames[0, 0].astype(jnp.float32)
            for p in range(1, phases):
                band = band + coef_re[:1, p:p + 1] * frames[0, p].astype(jnp.float32)
            parts = [band]
        else:
            coef_im = -level * unmix[order][1]
            band_re = coef_re[:1, 0:1] * frames[0, 0].astype(jnp.float32)
            band_im = coef_im[:1, 0:1] * frames[0, 0].astype(jnp.float32)
            for p in range(1, phases):
                f = frames[0, p].astype(jnp.float32)
                band_re = band_re + coef_re[:1, p:p + 1] * f
                band_im = band_im + coef_im[:1, p:p + 1] * f
            cx, sx, cy, sy = waves[order]
            ph_re = cy * cx - sy * sx
            ph_im = cy * sx + sy * cx
            parts = [band_re * ph_re - band_im * ph_im, band_re * ph_im + band_im * ph_re]
        for k, value in enumerate(parts):
            hi, lo = halves(value)
            planes[0, pl.ds((first + k) * rows, rows), :] = hi
            planes[1, pl.ds((first + k) * rows, rows), :] = lo
        span = pl.ds(first * rows, wide * rows)
        for c in far_chips:
            result = dot3(planes[0, span, :], planes[1, span, :], lead[0, c], lead[1, c])
            for k in range(wide):
                for kc in range(CORES):
                    send1[c * CORES + kc, :, pl.ds((first + k) * lanes, lanes)] = result[
                        k * rows:(k + 1) * rows, kc * lanes:(kc + 1) * lanes]
            for kc in range(CORES):
                send1_copy(c * CORES + kc, chip, core, me, g).start()
    mine = pl.ds(pl.multiple_of(core * rows, rows), rows)
    for g, (first, wide) in enumerate(groups):
        span = pl.ds(first * rows, wide * rows)
        result = dot3(planes[0, span, :], planes[1, span, :], lead[0, chip], lead[1, chip])
        for k in range(wide):
            block = result[k * rows:(k + 1) * rows]
            low_half, high_half = block[:, :lanes], block[:, lanes:]
            window = pl.ds((first + k) * lanes, lanes)
            recv1[chip, mine, window] = jnp.where(core == 0, low_half, high_half)
            send1[sibling, :, window] = jnp.where(core == 0, high_half, low_half)
        send1_copy(sibling, chip, core, me, g).start()

    for order in range(orders):
        make_weights(order)

    loads[1].wait()
    for g, (first, wide) in enumerate(groups):
        window = pl.ds(first * lanes, wide * lanes)
        send1_copy(sibling, chip, 1 - core, sibling, g).wait_recv()
        hi, lo = halves(recv1[chip, :, window])
        mixed[:, window] = dot3(column[0, chip], column[1, chip], hi, lo)
    for c in far_chips:
        for g, (first, wide) in enumerate(groups):
            window = pl.ds(first * lanes, wide * lanes)
            for kc in range(CORES):
                send1_copy(c * CORES + kc, c, kc, c * CORES + kc, g).wait_recv()
            hi, lo = halves(recv1[c, :, window])
            mixed[:, window] += dot3(column[0, c], column[1, c], hi, lo)

    lane = lax.broadcasted_iota(jnp.int32, (step, lanes), 1)
    low_lanes = lane < share
    special = jnp.logical_and(me == 0, jnp.logical_or(lane == 0, lane == share))
    special_top = jnp.logical_and(special, lane == share)
    freq_x = lane_freq((step, lanes))
    sign_x = jnp.where(low_lanes, 1.0, -1.0)
    parity_x = []
    for order in range(orders):
        turns = (placed(freq_x, order, shift_x) - freq_x) // pixels
        parity_x.append((1 - 2 * (turns & 1)).astype(jnp.float32))

    def turn_lanes(value):
        return pltpu.roll(value, share, 1)

    def combine(i, carry):
        first = pl.multiple_of(i * step, step)
        row0 = (first + lax.broadcasted_iota(jnp.int32, (step, lanes), 0)) == 0
        spectra = []
        for plane in range(phases):
            window = pl.ds(plane * lanes, lanes)
            upper = mixed[pl.ds(first, step), window]
            lower = mixed[pl.ds(half + first, step), window]
            upper_t, lower_t = turn_lanes(upper), turn_lanes(lower)
            as_is = jnp.logical_or(low_lanes, special)
            cc = jnp.where(as_is, upper, upper_t)
            sc = jnp.where(as_is, lower, lower_t)
            cs = jnp.where(special, 0.0, jnp.where(low_lanes, upper_t, upper)) * sign_x
            ss = jnp.where(special, 0.0, jnp.where(low_lanes, lower_t, lower)) * sign_x
            plus = (jnp.where(row0, cc, cc - ss), -jnp.where(row0, cs, sc + cs))
            minus = (jnp.where(row0, sc, cc + ss), jnp.where(row0, -ss, sc - cs))
            spectra.append((plus, minus))
        terms = []
        for sign in range(2):
            freq_y = row_freq(first, sign, (step, lanes))
            for order in range(orders):
                if order == 0:
                    re, im = spectra[phases - 1][sign]
                else:
                    rr, ri = spectra[2 * order - 2][sign]
                    ir, ii = spectra[2 * order - 1][sign]
                    re, im = rr - ii, ri + ir
                w = weights[order, sign, pl.ds(first, step), :]
                turns = (placed(freq_y, order, shift_y) - freq_y) // pixels
                terms.append((re * w, im * w, (1 - 2 * (turns & 1)).astype(jnp.float32)))
        for a in range(2):
            for b in range(2):
                sums = []
                for sign in range(2):
                    tot_re, tot_im = None, None
                    for order in range(orders):
                        re, im, par_y = terms[sign * orders + order]
                        factor = None
                        if a:
                            factor = par_y
                        if b:
                            factor = parity_x[order] if factor is None else factor * parity_x[order]
                        if factor is not None:
                            re, im = re * factor, im * factor
                        tot_re = re if tot_re is None else tot_re + re
                        tot_im = im if tot_im is None else tot_im + im
                    sums.append((tot_re, tot_im))
                (pr, pi), (mr, mi) = sums
                even_r = jnp.where(row0, pr, pr + mr)
                even_i = jnp.where(row0, pi, pi + mi)
                if a == 0:
                    odd_r = jnp.where(row0, mi, pr - mr)
                    odd_i = jnp.where(row0, -mr, pi - mi)
                else:
                    odd_r = jnp.where(row0, mr, pr - mr)
                    odd_i = jnp.where(row0, mi, pi - mi)

                def fold(x, y):
                    lo_val = x + turn_lanes(x)
                    hi_val = y - turn_lanes(y)
                    res = jnp.where(low_lanes, lo_val, hi_val)
                    res = jnp.where(special, x, res)
                    if b:
                        res = jnp.where(special_top, -y, res)
                    return res

                upper = fold(even_r, even_i)
                lower = fold(-odd_i, odd_r)
                window = pl.ds(b * lanes, lanes)
                hi, lo = halves(upper)
                coef[0, a, pl.ds(first, step), window] = hi
                coef[1, a, pl.ds(first, step), window] = lo
                hi, lo = halves(lower)
                coef[0, a, pl.ds(half + first, step), window] = hi
                coef[1, a, pl.ds(half + first, step), window] = lo
        return carry

    lax.fori_loop(0, half // step, combine, 0)

    def send2_copy(dest, slot_chip, slot_core, source, a):
        block = pl.ds(a * rows, rows)
        return pltpu.make_async_remote_copy(
            src_ref=send2.at[dest, :, block, :],
            dst_ref=recv2.at[slot_chip, :, block, pl.ds(pl.multiple_of(slot_core * lanes, lanes), lanes)],
            send_sem=ss2.at[dest, a], recv_sem=rs2.at[source, a],
            device_id={"row": dest}, device_id_type=MESH)

    loads[2].wait()
    for a in range(2):
        for _, dest in far:
            t = pl.ds(pl.multiple_of(dest * rows, rows), rows)
            result = dot3(inverse[0, a, t, :], inverse[1, a, t, :], coef[0, a], coef[1, a])
            for b in range(2):
                send2[dest, b, pl.ds(a * rows, rows), :] = result[:, b * lanes:(b + 1) * lanes]
            send2_copy(dest, chip, core, me, a).start()
    slot = pl.ds(pl.multiple_of(core * lanes, lanes), lanes)
    for a in range(2):
        for dest in (sibling, me):
            t = pl.ds(pl.multiple_of(dest * rows, rows), rows)
            result = dot3(inverse[0, a, t, :], inverse[1, a, t, :], coef[0, a], coef[1, a])
            for b in range(2):
                piece = result[:, b * lanes:(b + 1) * lanes]
                if dest is me:
                    recv2[chip, b, pl.ds(a * rows, rows), slot] = piece
                else:
                    send2[dest, b, pl.ds(a * rows, rows), :] = piece
            if dest is not me:
                send2_copy(dest, chip, core, me, a).start()

    loads[3].wait()
    for a in range(2):
        send2_copy(sibling, chip, 1 - core, sibling, a).wait_recv()
    wide_step = 256
    even_lane = (lax.broadcasted_iota(jnp.int32, (rows, wide_step), 1) & 1) == 0
    for stage, c in enumerate([chip] + far_chips):
        for a in range(2):
            if stage:
                for kc in range(CORES):
                    send2_copy(c * CORES + kc, c, kc, c * CORES + kc, a).wait_recv()
            block = pl.ds(a * rows, rows)
            for x in range(0, 2 * pixels, wide_step):
                span = pl.ds(x, wide_step)
                values = []
                for b in range(2):
                    hi, lo = halves(recv2[c, b, block, :])
                    values.append(dot3(hi, lo, last[0, c, :, span], last[1, c, :, span]))
                value = jnp.where(even_lane, values[0], values[1])
                place = pl.ds(a, rows, stride=2)
                for k in range(wide_step // 128):
                    piece = value[:, k * 128:(k + 1) * 128]
                    tile = x // 128 + k
                    if stage:
                        piece = piece + woven[tile, place, :]
                    woven[tile, place, :] = piece
    for tile in range(2 * pixels // 128):
        out[:, pl.ds(tile * 128, 128)] = woven[tile]

    for peer in others:
        tot_copy(peer, me).wait_send()
        for g in range(len(groups)):
            send1_copy(peer, chip, core, me, g).wait_send()
        for a in range(2):
            send2_copy(peer, chip, core, me, a).wait_send()


def solution(mesh):
    count = mesh.shape["row"]

    def per_device(frames, phase_offset, order_gain, band_shift):
        phases, rows, pixels = frames.shape[1:]
        lanes = pixels // count
        chips = count // CORES
        lead, column, inverse, last = tables(pixels, count)
        vmem = pl.BlockSpec(memory_space=pltpu.VMEM)
        smem = pl.BlockSpec(memory_space=pltpu.SMEM)
        hbm = pl.BlockSpec(memory_space=pl.ANY)
        bf16, f32 = jnp.bfloat16, jnp.float32
        dma = pltpu.SemaphoreType.DMA
        return pl.pallas_call(
            functools.partial(kernel, count, otf_polynomial()),
            out_shape=pltpu.VMEM((2 * rows, 2 * pixels), f32),
            in_specs=[vmem, smem, smem, smem, hbm, hbm, hbm, hbm],
            out_specs=vmem,
            scratch_shapes=[
                pltpu.VMEM(lead.shape, bf16),
                pltpu.VMEM(column.shape, bf16),
                pltpu.VMEM(inverse.shape, bf16),
                pltpu.VMEM(last.shape, bf16),
                pltpu.VMEM((8, 128), f32),
                pltpu.VMEM((count, 8, 128), f32),
                pltpu.VMEM((2, phases * rows, pixels), bf16),
                pltpu.VMEM((count, rows, phases * lanes), f32),
                pltpu.VMEM((chips, CORES * rows, phases * lanes), f32),
                pltpu.VMEM((pixels, phases * lanes), f32),
                pltpu.VMEM((phases // 2 + 1, 2, pixels // 2, lanes), f32),
                pltpu.VMEM((2, 2, pixels, 2 * lanes), bf16),
                pltpu.VMEM((count, 2, 2 * rows, lanes), f32),
                pltpu.VMEM((chips, 2, 2 * rows, CORES * lanes), f32),
                pltpu.VMEM((2 * pixels // 128, 2 * rows, 128), f32),
                dma((4,)),
                dma((count,)), dma((count,)),
                dma((count, 3)), dma((count, 3)),
                dma((count, 2)), dma((count, 2)),
            ],
            compiler_params=pltpu.CompilerParams(
                collective_id=0, has_side_effects=True, vmem_limit_bytes=60000000
            ),
        )(frames, phase_offset, order_gain, band_shift,
          jnp.asarray(lead), jnp.asarray(column), jnp.asarray(inverse), jnp.asarray(last))

    in_specs = (P("fov", None, "row", None), P("fov"), P("fov", None), P("fov", None))
    return jax.shard_map(
        per_device, mesh=mesh, in_specs=in_specs, out_specs=P(("fov", "row"), None), check_vma=False
    )
```
